32 devices in a mesh: dp: 8 (over z, x), tensor: 4 (over y, core).
Axes of the slice: x: 2, y: 2, z: 4, core: 2. Of those that a mesh axis runs over, the one named last changes fastest.
Arguments:
- inputs: bfloat16 [2, 2048, 1280], P(None, 'dp'), may hold values from -6 to 6
- cotangent: bfloat16 [2, 2048, 1280], P(None, 'dp'), may hold values from -0.625 to 0.625
- w_in: bfloat16 [1280, 5120], P('dp', 'tensor'), may hold values from -0.15625 to 0.15625
- w_out: bfloat16 [1280, 5120], P('dp', 'tensor'), may hold values from -0.078125 to 0.078125
- grad_in: float32 [1280, 5120], P('dp', 'tensor'), may hold values from -24 to 24
- grad_out: float32 [1280, 5120], P('dp', 'tensor'), may hold values from -24 to 24
Outputs:
- branch_output: bfloat16 [2, 2048, 1280], P(None, 'dp', 'tensor')
- ascent_in: float32 [1280, 5120], P('dp', 'tensor')
- ascent_out: float32 [1280, 5120], P('dp', 'tensor')
- new_grad_in: float32 [1280, 5120], P('dp', 'tensor')
- new_grad_out: float32 [1280, 5120], P('dp', 'tensor')
The draws below stay inside these ranges and needn't reach their ends.
All inputs are finite; a program needn't handle non-finite values.
Results may differ from the reference program's by a relative error of at most 0.0064.
Values may be sent and summed in bfloat16 or wider, within the bound.
A program may use at most 128 MiB of HBM per device.

```python
import math
import jax
import jax.numpy as jnp
from jax import lax

D = 1280
FF = 5120
MB = 2
TOKENS = 2048


def grad_table(key, rows, cols):
    key_rows, key_vals, key_common = jax.random.split(key, 3)
    scales = jnp.exp(jax.random.uniform(key_rows, (rows, 1), jnp.float32, math.log(0.25), math.log(4.0)))
    values = jnp.clip(jax.random.normal(key_vals, (rows, cols), jnp.float32), -6.0, 6.0)
    return jnp.clip(values * scales, -24.0, 24.0)


def draw_grad_in(key, part):
    return grad_table(jax.random.fold_in(key, 11), D, FF)


def draw_grad_out(key, part):
    return grad_table(jax.random.fold_in(key, 23), D, FF)


def with_spikes(values, rng, source, target, parts, factor):
    def block_of(position):
        return (jnp.arange(values.shape[position]) // (values.shape[position] // parts)).reshape((-1,) + (1,) * (values.ndim - 1 - position))

    one_side = jax.random.permutation(rng, parts)[block_of(target)]
    far = (block_of(target) + parts // 2) % parts
    return jnp.where((block_of(source) == one_side) | (block_of(source) == far), factor * values, values)


def shard_levels(key, dims, cuts, smallest, high):
    level = 1.0
    for dim, shards_of in cuts:
        draws = jax.random.uniform(jax.random.fold_in(jax.random.fold_in(key, 6), dim), (shards_of,), jnp.float32, smallest / len(cuts), high / len(cuts))
        level = level * jnp.repeat(jnp.exp(draws), dims[dim] // shards_of).reshape((-1,) + (1,) * (len(dims) - 1 - dim))
    return level


def noise(stream_key, extent, width, reach, cuts=(), held_as=jnp.bfloat16):
    values = width * jax.random.normal(stream_key, extent, jnp.float32)
    if cuts:
        values = values * shard_levels(stream_key, extent, cuts, -0.22, 0.18)
    return jnp.clip(values, -reach, reach).astype(held_as)


def bell_draw_with(stream_key, dims, spread, bound, pieces, heavy, kind=jnp.bfloat16):
    drawn = spread * jax.random.normal(stream_key, dims, jnp.float32)
    if pieces:
        drawn = drawn * shard_levels(stream_key, dims, pieces, -0.22, 0.18)
    return jnp.clip(with_spikes(drawn, jax.random.fold_in(stream_key, 3), *heavy), -bound, bound).astype(kind)


def setup_inputs(seed: int = 0) -> dict:
    splits = jax.random.split(jax.random.key(seed), 7)
    inputs = bell_draw_with(splits[0], (MB, TOKENS, D), 1.0, 6.0, ((1, 8),), (1, 2, 8, 2.0))
    cotangent = bell_draw_with(splits[1], (MB, TOKENS, D), (2.0 / (2 * TOKENS) ** 0.5), 0.625, ((1, 8),), (1, 2, 8, 2.0))
    w_in = noise(splits[2], (D, FF), D ** -0.5, 0.15625, ((0, 8), (1, 4)))
    w_out = noise(splits[3], (D, FF), FF ** -0.5, 0.078125, ((0, 8), (1, 4)))
    grad_in = draw_grad_in(jax.random.fold_in(splits[6], 71), 0)
    grad_out = draw_grad_out(jax.random.fold_in(splits[6], 71), 0)
    return {"inputs": inputs, "cotangent": cotangent, "w_in": w_in, "w_out": w_out, "grad_in": grad_in, "grad_out": grad_out}


RHO = 0.1
ETA = 0.01

def gelu_parts(pre):
    cdf = 0.5 * (1.0 + lax.erf(pre * 0.7071067811865476))
    dens = jnp.exp(-0.5 * pre * pre) * 0.3989422804014327
    return (pre * cdf, cdf + pre * dens)

def reference(inputs, cotangent, w_in, w_out, grad_in, grad_out):
    scale_in = jnp.abs(w_in.astype(jnp.float32)) + ETA
    scale_out = jnp.abs(w_out.astype(jnp.float32)) + ETA
    scaled_in = scale_in * grad_in
    scaled_out = scale_out * grad_out
    total = jnp.sum(scaled_in * scaled_in) + jnp.sum(scaled_out * scaled_out)
    factor = math.sqrt(2.0 * D * FF) / jnp.sqrt(total + 1.0)
    ascent_in = factor * scaled_in
    ascent_out = factor * scaled_out
    moved_in = (w_in.astype(jnp.float32) + RHO * scale_in * ascent_in).astype(jnp.bfloat16)
    moved_out = (w_out.astype(jnp.float32) + RHO * scale_out * ascent_out).astype(jnp.bfloat16)
    outputs = []
    new_in = jnp.zeros((D, FF), jnp.float32)
    new_out = jnp.zeros((D, FF), jnp.float32)
    for index in range(MB):
        rows = inputs[index]
        grads_y = cotangent[index]
        pre = jnp.dot(rows, moved_in, preferred_element_type=jnp.float32)
        act, slope = gelu_parts(pre)
        act = act.astype(jnp.bfloat16)
        result = jnp.dot(act, moved_out.T, preferred_element_type=jnp.float32)
        outputs.append(result.astype(jnp.bfloat16))
        back = jnp.dot(grads_y, moved_out, preferred_element_type=jnp.float32)
        delta = (back * slope).astype(jnp.bfloat16)
        new_in = new_in + jnp.dot(rows.T, delta, preferred_element_type=jnp.float32)
        new_out = new_out + jnp.dot(grads_y.T, act, preferred_element_type=jnp.float32)
    return (jnp.stack(outputs), ascent_in, ascent_out, new_in, new_out)
```

```python
import functools
import math

import jax
import jax.numpy as jnp
from jax import lax
from jax.experimental import pallas as pl
from jax.experimental.pallas import tpu as pltpu
from jax.sharding import PartitionSpec as P

D = 1280
FF = 5120


RHO = 0.1
ETA = 0.01


def gelu_parts(pre):
    cdf = 0.5 * (1.0 + lax.erf(pre * 0.7071067811865476))
    dens = jnp.exp(-0.5 * pre * pre) * 0.3989422804014327
    return (pre * cdf, cdf + pre * dens)


def token_product(left, right):
    return lax.dot_general(
        left, right, (((0,), (0,)), ((), ())), preferred_element_type=jnp.float32
    )


def local(inputs, cotangent, w_in, w_out, grad_in, grad_out):
    scale_in = jnp.abs(w_in.astype(jnp.float32)) + ETA
    scale_out = jnp.abs(w_out.astype(jnp.float32)) + ETA
    scaled_in = scale_in * grad_in
    scaled_out = scale_out * grad_out
    partial_sq = jnp.sum(scaled_in * scaled_in) + jnp.sum(scaled_out * scaled_out)
    row_total = lax.psum(partial_sq, "tensor")
    total = lax.psum(row_total, "dp")
    factor = math.sqrt(2.0 * D * FF) / jnp.sqrt(total + 1.0)
    ascent_in = factor * scaled_in
    ascent_out = factor * scaled_out
    moved_in = (w_in.astype(jnp.float32) + RHO * scale_in * ascent_in).astype(jnp.bfloat16)
    moved_out = (w_out.astype(jnp.float32) + RHO * scale_out * ascent_out).astype(jnp.bfloat16)
    micro = inputs.shape[0]
    full_in, full_out = (
        lax.all_gather(moved_in, "dp", axis=0, tiled=True),
        lax.all_gather(moved_out, "dp", axis=0, tiled=True),
    )
    outputs = []
    acts = []
    deltas = []
    for index in range(micro):
        rows = inputs[index]
        grads_y = cotangent[index]
        pre = jnp.dot(rows, full_in, preferred_element_type=jnp.float32)
        act, slope = gelu_parts(pre)
        act = act.astype(jnp.bfloat16)
        partial_y = lax.dot_general(
            act, full_out, (((1,), (1,)), ((), ())), preferred_element_type=jnp.float32
        )
        shared_y = lax.psum_scatter(partial_y, "tensor", scatter_dimension=1, tiled=True)
        outputs.append(shared_y.astype(jnp.bfloat16))
        back = jnp.dot(grads_y, full_out, preferred_element_type=jnp.float32)
        acts.append(act)
        deltas.append((back * slope).astype(jnp.bfloat16))
    branch_output = jnp.stack(outputs)
    flat_x = inputs.reshape(-1, inputs.shape[2])
    flat_dy = cotangent.reshape(-1, cotangent.shape[2])
    flat_delta = jnp.concatenate(deltas, axis=0)
    flat_act = jnp.concatenate(acts, axis=0)
    whole_in = token_product(flat_x, flat_delta)
    whole_out = token_product(flat_dy, flat_act)
    new_in, new_out = (
        lax.psum_scatter(whole_in, "dp", scatter_dimension=0, tiled=True),
        lax.psum_scatter(whole_out, "dp", scatter_dimension=0, tiled=True),
    )
    return (branch_output, ascent_in, ascent_out, new_in, new_out)


MESH = pl.DeviceIdType.MESH
GROUP = 4


def remote(src, dst, send, recv, where):
    copy = pltpu.make_async_remote_copy(
        src_ref=src, dst_ref=dst, send_sem=send, recv_sem=recv,
        device_id=where, device_id_type=MESH,
    )
    copy.start()
    return copy


def spread_kernel(dp, tp, const, pw, pc, sq, tok, wbuf, tbuf, tot,
                  sb1, sb2, mid, mv, s1, r1, s2, r2, ws, wr, ts, tr, ys, yr, cs, cr, loc):
    d = lax.axis_index("dp")
    t = lax.axis_index("tensor")
    g = lax.rem(d, GROUP)
    base = d - g
    copies = [
        remote(sq, sb1.at[k - 1], s1.at[k - 1], r1.at[k - 1], (d, lax.rem(t + k, tp)))
        for k in range(1, tp)
    ]
    own_tok = pltpu.make_async_copy(tok, tbuf.at[:, g], loc.at[0])
    own_tok.start()
    for copy in copies:
        copy.wait()
    part = sq[...]
    for k in range(tp - 1):
        part = part + sb1[k]
    mid[...] = part
    copies = [
        remote(mid, sb2.at[k - 1], s2.at[k - 1], r2.at[k - 1], (lax.rem(d + k, dp), t))
        for k in range(1, dp)
    ]
    for copy in copies:
        copy.wait()
    for k in range(dp - 1):
        part = part + sb2[k]
    tot[...] = part
    factor = const / jnp.sqrt(part[0:1, 0:1] + 1.0)
    for j in range(GROUP):
        mv[j] = (pw[j].astype(jnp.float32) + factor * pc[j]).astype(jnp.bfloat16)
    own_w = pltpu.make_async_copy(mv.at[g], wbuf.at[d], loc.at[1])
    own_w.start()
    order = sorted(range(1, dp), key=lambda k: abs(2 * k - dp))
    weights = []

    def send_weight(k):
        e = lax.rem(d + k, dp)
        weights.append(remote(mv.at[lax.rem(e, GROUP)], wbuf.at[d],
                              ws.at[k - 1], wr.at[k - 1], (e, t)))

    for k in order[:3]:
        send_weight(k)
    tokens = []
    for k in range(1, GROUP):
        p = lax.rem(g + k, GROUP)
        tokens.append(remote(tok.at[:, t], tbuf.at[:, g, t],
                             ts.at[k - 1], tr.at[k - 1], (base + p, t)))
    for k in order[3:]:
        send_weight(k)
    ty = lax.rem(t + tp // 2, tp)
    tc = t + 1 - 2 * lax.rem(t, 2)
    across = []
    beside = []
    for k in range(1, GROUP):
        q = lax.rem(g + GROUP - k, GROUP)
        tokens[k - 1].wait_recv()
        piece = tbuf.at[:, q, t]
        across.append(remote(piece, piece, ys.at[k - 1], yr.at[k - 1], (d, ty)))
        beside.append(remote(piece, piece, cs.at[k - 1], cr.at[k - 1], (d, tc)))
    for k in range(1, GROUP):
        q = lax.rem(g + GROUP - k, GROUP)
        across[k - 1].wait_recv()
        piece = tbuf.at[:, q, ty]
        beside.append(remote(piece, piece, cs.at[GROUP + k - 2], cr.at[GROUP + k - 2], (d, tc)))
    for copy in tokens + across:
        copy.wait_send()
    for copy in weights + beside:
        copy.wait()
    own_tok.wait()
    own_w.wait()


def spread(pw, pc, sq, tok, dp, tp, const):
    dma = lambda n: pltpu.SemaphoreType.DMA((n,))
    vm = pl.BlockSpec(memory_space=pltpu.VMEM)
    group, rows, cols = pw.shape
    return pl.pallas_call(
        functools.partial(spread_kernel, dp, tp, const),
        out_shape=(
            jax.ShapeDtypeStruct((dp, rows, cols), jnp.bfloat16),
            jax.ShapeDtypeStruct((tok.shape[0], group) + tok.shape[1:], jnp.bfloat16),
            jax.ShapeDtypeStruct((8, 128), jnp.float32),
        ),
        in_specs=[vm] * 4,
        out_specs=(vm, vm, vm),
        scratch_shapes=[
            pltpu.VMEM((tp - 1, 8, 128), jnp.float32),
            pltpu.VMEM((dp - 1, 8, 128), jnp.float32),
            pltpu.VMEM((8, 128), jnp.float32),
            pltpu.VMEM(pw.shape, jnp.bfloat16),
            dma(tp - 1), dma(tp - 1), dma(dp - 1), dma(dp - 1), dma(dp - 1), dma(dp - 1),
            dma(group - 1), dma(group - 1), dma(group - 1), dma(group - 1),
            dma(2 * group - 2), dma(2 * group - 2), dma(2),
        ],
        compiler_params=pltpu.CompilerParams(has_side_effects=True),
        name="spread",
    )(pw, pc, sq, tok)


def collect_kernel(dp, tp, pk, yt, grads, out,
                   gbuf, cb, yst, yb, z3, zb, gs, gr, cs, cr, ys, yr, zs, zr):
    d = lax.axis_index("dp")
    t = lax.axis_index("tensor")
    g = lax.rem(d, GROUP)
    base = d - g
    ty = lax.rem(t + tp // 2, tp)
    tc = t + 1 - 2 * lax.rem(t, 2)
    tcy = lax.rem(tc + tp // 2, tp)
    depth, width = yst.shape
    share = width // GROUP
    step = 32
    beside = [
        remote(yt.at[tcy], cb.at[1], cs.at[1], cr.at[1], (d, tc)),
        remote(yt.at[tc], cb.at[0], cs.at[0], cr.at[0], (d, tc)),
    ]
    sends = []
    for k in sorted(range(1, dp), key=lambda k: abs(2 * k - dp)):
        e = lax.rem(d + k, dp)
        sends.append(remote(pk.at[e], gbuf.at[k - 1], gs.at[k - 1], gr.at[k - 1], (e, t)))
    f32 = jnp.float32
    beside[0].wait()

    @pl.loop(0, depth // step)
    def _(i):
        at = pl.ds(pl.multiple_of(i * step, step), step)
        yst[at, :] = (yt[ty, at, :].astype(f32) + cb[1, at, :].astype(f32)).astype(jnp.bfloat16)

    across = remote(yst, yb, ys, yr, (d, ty))
    beside[1].wait()
    across.wait()

    @pl.loop(0, depth // step)
    def _(i):
        at = pl.ds(pl.multiple_of(i * step, step), step)
        whole = yt[t, at, :].astype(f32) + cb[0, at, :].astype(f32) + yb[at, :].astype(f32)
        for p in range(GROUP):
            z3[p, at, :] = whole[:, p * share:(p + 1) * share].astype(jnp.bfloat16)

    last = []
    for k in range(1, GROUP):
        p = lax.rem(g + k, GROUP)
        last.append(remote(z3.at[p], zb.at[k - 1], zs.at[k - 1], zr.at[k - 1], (base + p, t)))
    for copy in sends:
        copy.wait()
    for j in range(GROUP):
        total = None
        for k in range(j, dp, GROUP):
            piece = pk[d] if k == 0 else gbuf[k - 1]
            piece = piece.astype(f32)
            total = piece if total is None else total + piece
        grads[lax.rem(g + GROUP - j, GROUP)] = total
    for copy in last:
        copy.wait()

    @pl.loop(0, depth // step)
    def _(i):
        at = pl.ds(pl.multiple_of(i * step, step), step)
        whole = z3[g, at, :].astype(f32)
        for k in range(GROUP - 1):
            whole = whole + zb[k, at, :].astype(f32)
        out[at, :] = whole.astype(jnp.bfloat16)


def collect(pk, yt, dp, tp):
    dma = lambda n: pltpu.SemaphoreType.DMA((n,))
    vm = pl.BlockSpec(memory_space=pltpu.VMEM)
    _, rows, cols = pk.shape
    _, depth, width = yt.shape
    share = width // GROUP
    bf = jnp.bfloat16
    return pl.pallas_call(
        functools.partial(collect_kernel, dp, tp),
        out_shape=(
            jax.ShapeDtypeStruct((GROUP, rows, cols), jnp.float32),
            jax.ShapeDtypeStruct((depth, share), bf),
        ),
        in_specs=[vm] * 2,
        out_specs=(vm, vm),
        scratch_shapes=[
            pltpu.VMEM((dp - 1, rows, cols), bf),
            pltpu.VMEM((2, depth, width), bf),
            pltpu.VMEM((depth, width), bf),
            pltpu.VMEM((depth, width), bf),
            pltpu.VMEM((GROUP, depth, share), bf),
            pltpu.VMEM((GROUP - 1, depth, share), bf),
            dma(dp - 1), dma(dp - 1), dma(2), dma(2),
            pltpu.SemaphoreType.DMA, pltpu.SemaphoreType.DMA,
            dma(GROUP - 1), dma(GROUP - 1),
        ],
        compiler_params=pltpu.CompilerParams(has_side_effects=True),
        name="collect",
    )(pk, yt)


def regrouped(dp, tp, inputs, cotangent, w_in, w_out, grad_in, grad_out):
    f32, bf = jnp.float32, jnp.bfloat16
    micro, toks, width = inputs.shape
    rows, hidden = w_in.shape
    part = hidden // GROUP
    scale_in = jnp.abs(w_in.astype(f32)) + ETA
    scale_out = jnp.abs(w_out.astype(f32)) + ETA
    scaled_in = scale_in * grad_in
    scaled_out = scale_out * grad_out
    partial_sq = jnp.sum(scaled_in * scaled_in) + jnp.sum(scaled_out * scaled_out)

    def pack(a, b):
        a = a.reshape(rows, GROUP, part)
        b = b.reshape(rows, GROUP, part)
        return jnp.concatenate([a, b], axis=2).transpose(1, 0, 2)

    pw = pack(w_in, w_out)
    pc = pack(RHO * scale_in * scaled_in, RHO * scale_out * scaled_out)
    count = micro * toks
    tok = jnp.stack([inputs.reshape(tp, count // tp, width), cotangent.reshape(tp, count // tp, width)])
    const = math.sqrt(2.0 * rows * dp * hidden * tp)
    wbuf, tbuf, tot = spread(pw, pc, jnp.full((8, 128), partial_sq, f32), tok, dp, tp, const)
    factor = const / jnp.sqrt(tot[0, 0] + 1.0)
    ascent_in = factor * scaled_in
    ascent_out = factor * scaled_out
    full = wbuf.reshape(rows * dp, 2 * part)
    full_in, full_out = full[:, :part], full[:, part:]
    flat_x = tbuf[0].reshape(GROUP * count, width)
    flat_dy = tbuf[1].reshape(GROUP * count, width)
    pre = jnp.dot(flat_x, full_in, preferred_element_type=f32)
    act, slope = gelu_parts(pre)
    act = act.astype(bf)
    yt = lax.dot_general(full_out, act, (((1,), (1,)), ((), ())), preferred_element_type=f32)
    yt = yt.astype(bf).reshape(tp, width // tp, GROUP * count)
    back = jnp.dot(flat_dy, full_out, preferred_element_type=f32)
    delta = (back * slope).astype(bf)
    packed = jnp.concatenate(
        [token_product(flat_x, delta), token_product(flat_dy, act)], axis=1
    ).astype(bf).reshape(dp, rows, 2 * part)
    grads, out = collect(packed, yt, dp, tp)
    branch = out.T.reshape(micro, toks, width // tp)
    new_in = grads[:, :, :part].transpose(1, 0, 2).reshape(rows, hidden)
    new_out = grads[:, :, part:].transpose(1, 0, 2).reshape(rows, hidden)
    return (branch, ascent_in, ascent_out, new_in, new_out)


def body(dp, tp, inputs, cotangent, w_in, *rest):
    micro, toks, width = inputs.shape
    rows, hidden = w_in.shape
    fits = (
        tp == 4 and dp % GROUP == 0 and rows % 16 == 0
        and hidden % (64 * GROUP) == 0 and (micro * toks) % 128 == 0
        and width % (32 * tp) == 0
    )
    if fits:
        return regrouped(dp, tp, inputs, cotangent, w_in, *rest)
    return local(inputs, cotangent, w_in, *rest)


def solution(mesh):
    return jax.shard_map(
        functools.partial(body, mesh.shape["dp"], mesh.shape["tensor"]),
        mesh=mesh,
        in_specs=(
            P(None, "dp", None),
            P(None, "dp", None),
            P("dp", "tensor"),
            P("dp", "tensor"),
            P("dp", "tensor"),
            P("dp", "tensor"),
        ),
        out_specs=(
            P(None, "dp", "tensor"),
            P("dp", "tensor"),
            P("dp", "tensor"),
            P("dp", "tensor"),
            P("dp", "tensor"),
        ),
        check_vma=False,
    )
```

```python
import functools
import math

import jax
import jax.numpy as jnp
from jax import lax
from jax.experimental import pallas as pl
from jax.experimental.pallas import tpu as pltpu
from jax.sharding import PartitionSpec as P

D = 1280
FF = 5120


RHO = 0.1
ETA = 0.01


def gelu_parts(pre):
    cdf = 0.5 * (1.0 + lax.erf(pre * 0.7071067811865476))
    dens = jnp.exp(-0.5 * pre * pre) * 0.3989422804014327
    return (pre * cdf, cdf + pre * dens)


def token_product(left, right):
    return lax.dot_general(
        left, right, (((0,), (0,)), ((), ())), preferred_element_type=jnp.float32
    )


def local(inputs, cotangent, w_in, w_out, grad_in, grad_out):
    scale_in = jnp.abs(w_in.astype(jnp.float32)) + ETA
    scale_out = jnp.abs(w_out.astype(jnp.float32)) + ETA
    scaled_in = scale_in * grad_in
    scaled_out = scale_out * grad_out
    partial_sq = jnp.sum(scaled_in * scaled_in) + jnp.sum(scaled_out * scaled_out)
    row_total = lax.psum(partial_sq, "tensor")
    total = lax.psum(row_total, "dp")
    factor = math.sqrt(2.0 * D * FF) / jnp.sqrt(total + 1.0)
    ascent_in = factor * scaled_in
    ascent_out = factor * scaled_out
    moved_in = (w_in.astype(jnp.float32) + RHO * scale_in * ascent_in).astype(jnp.bfloat16)
    moved_out = (w_out.astype(jnp.float32) + RHO * scale_out * ascent_out).astype(jnp.bfloat16)
    micro = inputs.shape[0]
    full_in, full_out = (
        lax.all_gather(moved_in, "dp", axis=0, tiled=True),
        lax.all_gather(moved_out, "dp", axis=0, tiled=True),
    )
    outputs = []
    acts = []
    deltas = []
    for index in range(micro):
        rows = inputs[index]
        grads_y = cotangent[index]
        pre = jnp.dot(rows, full_in, preferred_element_type=jnp.float32)
        act, slope = gelu_parts(pre)
        act = act.astype(jnp.bfloat16)
        partial_y = lax.dot_general(
            act, full_out, (((1,), (1,)), ((), ())), preferred_element_type=jnp.float32
        )
        shared_y = lax.psum_scatter(partial_y, "tensor", scatter_dimension=1, tiled=True)
        outputs.append(shared_y.astype(jnp.bfloat16))
        back = jnp.dot(grads_y, full_out, preferred_element_type=jnp.float32)
        acts.append(act)
        deltas.append((back * slope).astype(jnp.bfloat16))
    branch_output = jnp.stack(outputs)
    flat_x = inputs.reshape(-1, inputs.shape[2])
    flat_dy = cotangent.reshape(-1, cotangent.shape[2])
    flat_delta = jnp.concatenate(deltas, axis=0)
    flat_act = jnp.concatenate(acts, axis=0)
    whole_in = token_product(flat_x, flat_delta)
    whole_out = token_product(flat_dy, flat_act)
    new_in, new_out = (
        lax.psum_scatter(whole_in, "dp", scatter_dimension=0, tiled=True),
        lax.psum_scatter(whole_out, "dp", scatter_dimension=0, tiled=True),
    )
    return (branch_output, ascent_in, ascent_out, new_in, new_out)


MESH = pl.DeviceIdType.MESH
GROUP = 4


def remote(src, dst, send, recv, where):
    copy = pltpu.make_async_remote_copy(
        src_ref=src, dst_ref=dst, send_sem=send, recv_sem=recv,
        device_id=where, device_id_type=MESH,
    )
    copy.start()
    return copy


def spread_kernel(dp, tp, const, pw, pc, sq, tx, tdy, wbuf, xbuf, dbuf, tot,
                  sb1, sb2, mid, mv, s1, r1, s2, r2, ws, wr, ts, tr, ys, yr, cs, cr, loc):
    d = lax.axis_index("dp")
    t = lax.axis_index("tensor")
    g = lax.rem(d, GROUP)
    base = d - g
    copies = [
        remote(sq, sb1.at[k - 1], s1.at[k - 1], r1.at[k - 1], (d, lax.rem(t + k, tp)))
        for k in range(1, tp)
    ]
    pairs = ((tx, xbuf), (tdy, dbuf))
    own = [
        pltpu.make_async_copy(src, buf.at[g], loc.at[i]) for i, (src, buf) in enumerate(pairs)
    ]
    for copy in own:
        copy.start()
    for copy in copies:
        copy.wait()
    part = sq[...]
    for k in range(tp - 1):
        part = part + sb1[k]
    mid[...] = part
    copies = [
        remote(mid, sb2.at[k - 1], s2.at[k - 1], r2.at[k - 1], (lax.rem(d + k, dp), t))
        for k in range(1, dp)
    ]
    tokens = []
    for k in range(1, GROUP):
        p = lax.rem(g + k, GROUP)
        for i, (src, buf) in enumerate(pairs):
            n = 2 * k - 2 + i
            tokens.append(remote(src.at[t], buf.at[g, t], ts.at[n], tr.at[n], (base + p, t)))
    for copy in copies:
        copy.wait()
    for k in range(dp - 1):
        part = part + sb2[k]
    tot[...] = part
    factor = const / jnp.sqrt(part[0:1, 0:1] + 1.0)
    for j in range(GROUP):
        mv[j] = (pw[j].astype(jnp.float32) + factor * pc[j]).astype(jnp.bfloat16)
    own_w = pltpu.make_async_copy(mv.at[g], wbuf.at[d], loc.at[2])
    own_w.start()
    order = sorted(range(1, dp), key=lambda k: abs(2 * k - dp))
    weights = []

    def send_weight(k):
        e = lax.rem(d + k, dp)
        weights.append(remote(mv.at[lax.rem(e, GROUP)], wbuf.at[d],
                              ws.at[k - 1], wr.at[k - 1], (e, t)))

    for k in order:
        send_weight(k)
    ty = lax.rem(t + tp // 2, tp)
    tc = t + 1 - 2 * lax.rem(t, 2)
    across = []
    beside = []
    moves = 2 * GROUP - 2
    for n in range(moves):
        q = lax.rem(g + GROUP - (n // 2 + 1), GROUP)
        tokens[n].wait_recv()
        piece = pairs[n % 2][1].at[q, t]
        across.append(remote(piece, piece, ys.at[n], yr.at[n], (d, ty)))
        beside.append(remote(piece, piece, cs.at[n], cr.at[n], (d, tc)))
    for n in range(moves):
        q = lax.rem(g + GROUP - (n // 2 + 1), GROUP)
        across[n].wait_recv()
        piece = pairs[n % 2][1].at[q, ty]
        beside.append(remote(piece, piece, cs.at[moves + n], cr.at[moves + n], (d, tc)))
    for copy in tokens + across:
        copy.wait_send()
    for copy in weights + beside:
        copy.wait()
    for copy in own:
        copy.wait()
    own_w.wait()


def spread(pw, pc, sq, tx, tdy, dp, tp, const):
    dma = lambda n: pltpu.SemaphoreType.DMA((n,))
    vm = pl.BlockSpec(memory_space=pltpu.VMEM)
    group, rows, cols = pw.shape
    return pl.pallas_call(
        functools.partial(spread_kernel, dp, tp, const),
        out_shape=(
            jax.ShapeDtypeStruct((dp, rows, cols), jnp.bfloat16),
            jax.ShapeDtypeStruct((group,) + tx.shape, jnp.bfloat16),
            jax.ShapeDtypeStruct((group,) + tdy.shape, jnp.bfloat16),
            jax.ShapeDtypeStruct((8, 128), jnp.float32),
        ),
        in_specs=[vm] * 5,
        out_specs=(vm, vm, vm, vm),
        scratch_shapes=[
            pltpu.VMEM((tp - 1, 8, 128), jnp.float32),
            pltpu.VMEM((dp - 1, 8, 128), jnp.float32),
            pltpu.VMEM((8, 128), jnp.float32),
            pltpu.VMEM(pw.shape, jnp.bfloat16),
            dma(tp - 1), dma(tp - 1), dma(dp - 1), dma(dp - 1), dma(dp - 1), dma(dp - 1),
            dma(2 * group - 2), dma(2 * group - 2), dma(2 * group - 2), dma(2 * group - 2),
            dma(4 * group - 4), dma(4 * group - 4), dma(3),
        ],
        compiler_params=pltpu.CompilerParams(has_side_effects=True),
        name="spread",
    )(pw, pc, sq, tx, tdy)


def collect_kernel(dp, tp, pk, yt, new_in, new_out, out,
                   gbuf, cb, yst, yb, z3, zb, gs, gr, cs, cr, ys, yr, zs, zr, loc):
    d = lax.axis_index("dp")
    t = lax.axis_index("tensor")
    g = lax.rem(d, GROUP)
    base = d - g
    ty = lax.rem(t + tp // 2, tp)
    tc = t + 1 - 2 * lax.rem(t, 2)
    tcy = lax.rem(tc + tp // 2, tp)
    depth, width = yst.shape
    share = width // GROUP
    step = 32
    beside = [
        remote(yt.at[tcy], cb.at[1], cs.at[1], cr.at[1], (d, tc)),
        remote(yt.at[tc], cb.at[0], cs.at[0], cr.at[0], (d, tc)),
    ]
    sends = []
    for k in sorted(range(1, dp), key=lambda k: abs(2 * k - dp)):
        e = lax.rem(d + k, dp)
        sends.append(remote(pk.at[e], gbuf.at[d], gs.at[k - 1], gr.at[k - 1], (e, t)))
    f32 = jnp.float32
    own = pltpu.make_async_copy(pk.at[d], gbuf.at[d], loc)
    own.start()
    beside[0].wait()

    @pl.loop(0, depth // step)
    def _(i):
        at = pl.ds(pl.multiple_of(i * step, step), step)
        yst[at, :] = (yt[ty, at, :].astype(f32) + cb[1, at, :].astype(f32)).astype(jnp.bfloat16)

    across = remote(yst, yb, ys, yr, (d, ty))
    beside[1].wait()
    across.wait()

    @pl.loop(0, depth // step)
    def _(i):
        at = pl.ds(pl.multiple_of(i * step, step), step)
        whole = yt[t, at, :].astype(f32) + cb[0, at, :].astype(f32) + yb[at, :].astype(f32)
        for p in range(GROUP):
            z3[p, at, :] = whole[:, p * share:(p + 1) * share].astype(jnp.bfloat16)

    last = []
    for k in range(1, GROUP):
        p = lax.rem(g + k, GROUP)
        last.append(remote(z3.at[p], zb.at[k - 1], zs.at[k - 1], zr.at[k - 1], (base + p, t)))
    for copy in sends:
        copy.wait()
    own.wait()
    part = pk.shape[2] // 2
    for j in range(GROUP):
        total = gbuf[j].astype(f32)
        for e in range(j + GROUP, dp, GROUP):
            total = total + gbuf[e].astype(f32)
        new_in[:, j * part:(j + 1) * part] = total[:, :part]
        new_out[:, j * part:(j + 1) * part] = total[:, part:]
    for copy in last:
        copy.wait()

    @pl.loop(0, depth // step)
    def _(i):
        at = pl.ds(pl.multiple_of(i * step, step), step)
        whole = z3[g, at, :].astype(f32)
        for k in range(GROUP - 1):
            whole = whole + zb[k, at, :].astype(f32)
        out[at, :] = whole.astype(jnp.bfloat16)


def collect(pk, yt, dp, tp):
    dma = lambda n: pltpu.SemaphoreType.DMA((n,))
    vm = pl.BlockSpec(memory_space=pltpu.VMEM)
    _, rows, cols = pk.shape
    _, depth, width = yt.shape
    share = width // GROUP
    bf = jnp.bfloat16
    return pl.pallas_call(
        functools.partial(collect_kernel, dp, tp),
        out_shape=(
            jax.ShapeDtypeStruct((rows, GROUP * cols // 2), jnp.float32),
            jax.ShapeDtypeStruct((rows, GROUP * cols // 2), jnp.float32),
            jax.ShapeDtypeStruct((depth, share), bf),
        ),
        in_specs=[vm] * 2,
        out_specs=(vm, vm, vm),
        scratch_shapes=[
            pltpu.VMEM((dp, rows, cols), bf),
            pltpu.VMEM((2, depth, width), bf),
            pltpu.VMEM((depth, width), bf),
            pltpu.VMEM((depth, width), bf),
            pltpu.VMEM((GROUP, depth, share), bf),
            pltpu.VMEM((GROUP - 1, depth, share), bf),
            dma(dp - 1), dma(dp - 1), dma(2), dma(2),
            pltpu.SemaphoreType.DMA, pltpu.SemaphoreType.DMA,
            dma(GROUP - 1), dma(GROUP - 1), pltpu.SemaphoreType.DMA,
        ],
        compiler_params=pltpu.CompilerParams(has_side_effects=True),
        name="collect",
    )(pk, yt)


def regrouped(dp, tp, inputs, cotangent, w_in, w_out, grad_in, grad_out):
    f32, bf = jnp.float32, jnp.bfloat16
    micro, toks, width = inputs.shape
    rows, hidden = w_in.shape
    part = hidden // GROUP
    scale_in = jnp.abs(w_in.astype(f32)) + ETA
    scale_out = jnp.abs(w_out.astype(f32)) + ETA
    scaled_in = scale_in * grad_in
    scaled_out = scale_out * grad_out
    partial_sq = jnp.sum(scaled_in * scaled_in) + jnp.sum(scaled_out * scaled_out)

    def pack(a, b):
        a = a.reshape(rows, GROUP, part)
        b = b.reshape(rows, GROUP, part)
        return jnp.concatenate([a, b], axis=2).transpose(1, 0, 2)

    pw = pack(w_in, w_out)
    pc = pack(RHO * scale_in * scaled_in, RHO * scale_out * scaled_out)
    count = micro * toks
    tx = inputs.reshape(tp, count // tp, width)
    tdy = cotangent.reshape(tp, count // tp, width)
    const = math.sqrt(2.0 * rows * dp * hidden * tp)
    wbuf, xbuf, dbuf, tot = spread(
        pw, pc, jnp.full((8, 128), partial_sq, f32), tx, tdy, dp, tp, const
    )
    factor = const / jnp.sqrt(tot[0, 0] + 1.0)
    ascent_in = factor * scaled_in
    ascent_out = factor * scaled_out
    full = wbuf.reshape(rows * dp, 2 * part)
    full_in, full_out = full[:, :part], full[:, part:]
    flat_x = xbuf.reshape(GROUP * count, width)
    flat_dy = dbuf.reshape(GROUP * count, width)

    def against(weight, tokens):
        return lax.dot_general(weight, tokens, (((0,), (1,)), ((), ())), preferred_element_type=f32)

    act, slope = gelu_parts(against(full_in, flat_x))
    act = act.astype(bf)
    yt = jnp.dot(full_out, act, preferred_element_type=f32)
    yt = yt.astype(bf).reshape(tp, width // tp, GROUP * count)
    delta = (against(full_out, flat_dy) * slope).astype(bf)
    packed = jnp.concatenate([
        jnp.dot(delta, flat_x, preferred_element_type=f32).astype(bf),
        jnp.dot(act, flat_dy, preferred_element_type=f32).astype(bf),
    ], axis=0).T.reshape(dp, rows, 2 * part)
    new_in, new_out, out = collect(packed, yt, dp, tp)
    branch = out.T.reshape(micro, toks, width // tp)
    return (branch, ascent_in, ascent_out, new_in, new_out)


def body(dp, tp, inputs, cotangent, w_in, *rest):
    micro, toks, width = inputs.shape
    rows, hidden = w_in.shape
    fits = (
        tp == 4 and dp % GROUP == 0 and rows % 16 == 0
        and hidden % (64 * GROUP) == 0 and (micro * toks) % 128 == 0
        and width % (32 * tp) == 0
    )
    if fits:
        return regrouped(dp, tp, inputs, cotangent, w_in, *rest)
    return local(inputs, cotangent, w_in, *rest)


def solution(mesh):
    return jax.shard_map(
        functools.partial(body, mesh.shape["dp"], mesh.shape["tensor"]),
        mesh=mesh,
        in_specs=(
            P(None, "dp", None),
            P(None, "dp", None),
            P("dp", "tensor"),
            P("dp", "tensor"),
            P("dp", "tensor"),
            P("dp", "tensor"),
        ),
        out_specs=(
            P(None, "dp", "tensor"),
            P("dp", "tensor"),
            P("dp", "tensor"),
            P("dp", "tensor"),
            P("dp", "tensor"),
        ),
        check_vma=False,
    )
```

```python
import functools
import math

import jax
import jax.numpy as jnp
from jax import lax
from jax.experimental import pallas as pl
from jax.experimental.pallas import tpu as pltpu
from jax.sharding import PartitionSpec as P

D = 1280
FF = 5120


RHO = 0.1
ETA = 0.01


def gelu_parts(pre):
    cdf = 0.5 * (1.0 + lax.erf(pre * 0.7071067811865476))
    dens = jnp.exp(-0.5 * pre * pre) * 0.3989422804014327
    return (pre * cdf, cdf + pre * dens)


def token_product(left, right):
    return lax.dot_general(
        left, right, (((0,), (0,)), ((), ())), preferred_element_type=jnp.float32
    )


def local(inputs, cotangent, w_in, w_out, grad_in, grad_out):
    scale_in = jnp.abs(w_in.astype(jnp.float32)) + ETA
    scale_out = jnp.abs(w_out.astype(jnp.float32)) + ETA
    scaled_in = scale_in * grad_in
    scaled_out = scale_out * grad_out
    partial_sq = jnp.sum(scaled_in * scaled_in) + jnp.sum(scaled_out * scaled_out)
    row_total = lax.psum(partial_sq, "tensor")
    total = lax.psum(row_total, "dp")
    factor = math.sqrt(2.0 * D * FF) / jnp.sqrt(total + 1.0)
    ascent_in = factor * scaled_in
    ascent_out = factor * scaled_out
    moved_in = (w_in.astype(jnp.float32) + RHO * scale_in * ascent_in).astype(jnp.bfloat16)
    moved_out = (w_out.astype(jnp.float32) + RHO * scale_out * ascent_out).astype(jnp.bfloat16)
    micro = inputs.shape[0]
    full_in, full_out = (
        lax.all_gather(moved_in, "dp", axis=0, tiled=True),
        lax.all_gather(moved_out, "dp", axis=0, tiled=True),
    )
    outputs = []
    acts = []
    deltas = []
    for index in range(micro):
        rows = inputs[index]
        grads_y = cotangent[index]
        pre = jnp.dot(rows, full_in, preferred_element_type=jnp.float32)
        act, slope = gelu_parts(pre)
        act = act.astype(jnp.bfloat16)
        partial_y = lax.dot_general(
            act, full_out, (((1,), (1,)), ((), ())), preferred_element_type=jnp.float32
        )
        shared_y = lax.psum_scatter(partial_y, "tensor", scatter_dimension=1, tiled=True)
        outputs.append(shared_y.astype(jnp.bfloat16))
        back = jnp.dot(grads_y, full_out, preferred_element_type=jnp.float32)
        acts.append(act)
        deltas.append((back * slope).astype(jnp.bfloat16))
    branch_output = jnp.stack(outputs)
    flat_x = inputs.reshape(-1, inputs.shape[2])
    flat_dy = cotangent.reshape(-1, cotangent.shape[2])
    flat_delta = jnp.concatenate(deltas, axis=0)
    flat_act = jnp.concatenate(acts, axis=0)
    whole_in = token_product(flat_x, flat_delta)
    whole_out = token_product(flat_dy, flat_act)
    new_in, new_out = (
        lax.psum_scatter(whole_in, "dp", scatter_dimension=0, tiled=True),
        lax.psum_scatter(whole_out, "dp", scatter_dimension=0, tiled=True),
    )
    return (branch_output, ascent_in, ascent_out, new_in, new_out)


MESH = pl.DeviceIdType.MESH
GROUP = 4


def remote(src, dst, send, recv, where):
    copy = pltpu.make_async_remote_copy(
        src_ref=src, dst_ref=dst, send_sem=send, recv_sem=recv,
        device_id=where, device_id_type=MESH,
    )
    copy.start()
    return copy


def spread_kernel(dp, tp, const, pw, pc, sq, tx, tdy, wbuf, xbuf, dbuf, tot,
                  sb1, sb2, mid, mv, s1, r1, s2, r2, ws, wr, ts, tr, ys, yr, cs, cr, loc):
    d = lax.axis_index("dp")
    t = lax.axis_index("tensor")
    g = lax.rem(d, GROUP)
    base = d - g
    copies = [
        remote(sq, sb1.at[k - 1], s1.at[k - 1], r1.at[k - 1], (d, lax.rem(t + k, tp)))
        for k in range(1, tp)
    ]
    pairs = ((tx, xbuf), (tdy, dbuf))
    own = [
        pltpu.make_async_copy(src, buf.at[g], loc.at[i]) for i, (src, buf) in enumerate(pairs)
    ]
    for copy in own:
        copy.start()
    for copy in copies:
        copy.wait()
    part = sq[...]
    for k in range(tp - 1):
        part = part + sb1[k]
    mid[...] = part
    copies = [
        remote(mid, sb2.at[k - 1], s2.at[k - 1], r2.at[k - 1], (lax.rem(d + k, dp), t))
        for k in range(1, dp)
    ]
    tokens = []
    for k in range(1, GROUP):
        p = lax.rem(g + k, GROUP)
        for i, (src, buf) in enumerate(pairs):
            n = 2 * k - 2 + i
            tokens.append(remote(src.at[t], buf.at[g, t], ts.at[n], tr.at[n], (base + p, t)))
    for copy in copies:
        copy.wait()
    for k in range(dp - 1):
        part = part + sb2[k]
    tot[...] = part
    factor = const / jnp.sqrt(part[0:1, 0:1] + 1.0)
    for j in range(GROUP):
        mv[j] = (pw[j].astype(jnp.float32) + factor * pc[j]).astype(jnp.bfloat16)
    own_w = pltpu.make_async_copy(mv.at[g], wbuf.at[d], loc.at[2])
    own_w.start()
    order = sorted(range(1, dp), key=lambda k: abs(2 * k - dp))
    weights = []

    def send_weight(k):
        e = lax.rem(d + k, dp)
        weights.append(remote(mv.at[lax.rem(e, GROUP)], wbuf.at[d],
                              ws.at[k - 1], wr.at[k - 1], (e, t)))

    for k in order:
        send_weight(k)
    ty = lax.rem(t + tp // 2, tp)
    tc = t + 1 - 2 * lax.rem(t, 2)
    across = []
    beside = []
    moves = 2 * GROUP - 2
    for n in range(moves):
        q = lax.rem(g + GROUP - (n // 2 + 1), GROUP)
        tokens[n].wait_recv()
        piece = pairs[n % 2][1].at[q, t]
        across.append(remote(piece, piece, ys.at[n], yr.at[n], (d, ty)))
        beside.append(remote(piece, piece, cs.at[n], cr.at[n], (d, tc)))
    for n in range(moves):
        q = lax.rem(g + GROUP - (n // 2 + 1), GROUP)
        across[n].wait_recv()
        piece = pairs[n % 2][1].at[q, ty]
        beside.append(remote(piece, piece, cs.at[moves + n], cr.at[moves + n], (d, tc)))
    for copy in tokens + across:
        copy.wait_send()
    for copy in weights + beside:
        copy.wait()
    for copy in own:
        copy.wait()
    own_w.wait()


def spread(pw, pc, sq, tx, tdy, dp, tp, const):
    dma = lambda n: pltpu.SemaphoreType.DMA((n,))
    vm = pl.BlockSpec(memory_space=pltpu.VMEM)
    group, rows, cols = pw.shape
    return pl.pallas_call(
        functools.partial(spread_kernel, dp, tp, const),
        out_shape=(
            jax.ShapeDtypeStruct((dp, rows, cols), jnp.bfloat16),
            jax.ShapeDtypeStruct((group,) + tx.shape, jnp.bfloat16),
            jax.ShapeDtypeStruct((group,) + tdy.shape, jnp.bfloat16),
            jax.ShapeDtypeStruct((8, 128), jnp.float32),
        ),
        in_specs=[vm] * 5,
        out_specs=(vm, vm, vm, vm),
        scratch_shapes=[
            pltpu.VMEM((tp - 1, 8, 128), jnp.float32),
            pltpu.VMEM((dp - 1, 8, 128), jnp.float32),
            pltpu.VMEM((8, 128), jnp.float32),
            pltpu.VMEM(pw.shape, jnp.bfloat16),
            dma(tp - 1), dma(tp - 1), dma(dp - 1), dma(dp - 1), dma(dp - 1), dma(dp - 1),
            dma(2 * group - 2), dma(2 * group - 2), dma(2 * group - 2), dma(2 * group - 2),
            dma(4 * group - 4), dma(4 * group - 4), dma(3),
        ],
        compiler_params=pltpu.CompilerParams(has_side_effects=True),
        name="spread",
    )(pw, pc, sq, tx, tdy)


def collect_kernel(dp, tp, pk, yt, new_in, new_out, out,
                   gbuf, cb, yst, yb, z3, zb, gs, gr, cs, cr, ys, yr, zs, zr, loc):
    d = lax.axis_index("dp")
    t = lax.axis_index("tensor")
    g = lax.rem(d, GROUP)
    base = d - g
    ty = lax.rem(t + tp // 2, tp)
    tc = t + 1 - 2 * lax.rem(t, 2)
    tcy = lax.rem(tc + tp // 2, tp)
    _, depth, share = yst.shape
    step = 32
    order = list(range(1, GROUP)) + [0]
    columns = [pl.ds(pl.multiple_of(lax.rem(g + k, GROUP) * share, share), share) for k in range(GROUP)]
    beside = [{}, {}]
    for half, whose in ((1, tcy), (0, tc)):
        for k in order:
            n = half * GROUP + k
            beside[half][k] = remote(
                yt.at[whose, :, columns[k]], cb.at[half, k], cs.at[n], cr.at[n], (d, tc)
            )
    sends = []
    for k in sorted(range(1, dp), key=lambda k: abs(2 * k - dp)):
        e = lax.rem(d + k, dp)
        sends.append(remote(pk.at[e], gbuf.at[d], gs.at[k - 1], gr.at[k - 1], (e, t)))
    f32 = jnp.float32
    own = pltpu.make_async_copy(pk.at[d], gbuf.at[d], loc)
    own.start()
    across = {}
    for k in order:
        beside[1][k].wait()

        @pl.loop(0, depth // step)
        def _(i):
            at = pl.ds(pl.multiple_of(i * step, step), step)
            whole = yt[ty, at, columns[k]].astype(f32) + cb[1, k, at, :].astype(f32)
            yst[k, at, :] = whole.astype(jnp.bfloat16)

        across[k] = remote(yst.at[k], yb.at[k], ys.at[k], yr.at[k], (d, ty))
    last = []
    for k in order:
        beside[0][k].wait()
        across[k].wait()

        @pl.loop(0, depth // step)
        def _(i):
            at = pl.ds(pl.multiple_of(i * step, step), step)
            whole = yt[t, at, columns[k]].astype(f32) + cb[0, k, at, :].astype(f32)
            z3[k, at, :] = (whole + yb[k, at, :].astype(f32)).astype(jnp.bfloat16)

        if k > 0:
            p = lax.rem(g + k, GROUP)
            last.append(remote(z3.at[k], zb.at[k - 1], zs.at[k - 1], zr.at[k - 1], (base + p, t)))
    for copy in sends:
        copy.wait()
    own.wait()
    part = pk.shape[2] // 2
    for j in range(GROUP):
        total = gbuf[j].astype(f32)
        for e in range(j + GROUP, dp, GROUP):
            total = total + gbuf[e].astype(f32)
        new_in[:, j * part:(j + 1) * part] = total[:, :part]
        new_out[:, j * part:(j + 1) * part] = total[:, part:]
    for copy in last:
        copy.wait()

    @pl.loop(0, depth // step)
    def _(i):
        at = pl.ds(pl.multiple_of(i * step, step), step)
        whole = z3[0, at, :].astype(f32)
        for k in range(GROUP - 1):
            whole = whole + zb[k, at, :].astype(f32)
        out[at, :] = whole.astype(jnp.bfloat16)


def collect(pk, yt, dp, tp):
    dma = lambda n: pltpu.SemaphoreType.DMA((n,))
    vm = pl.BlockSpec(memory_space=pltpu.VMEM)
    _, rows, cols = pk.shape
    _, depth, width = yt.shape
    share = width // GROUP
    bf = jnp.bfloat16
    return pl.pallas_call(
        functools.partial(collect_kernel, dp, tp),
        out_shape=(
            jax.ShapeDtypeStruct((rows, GROUP * cols // 2), jnp.float32),
            jax.ShapeDtypeStruct((rows, GROUP * cols // 2), jnp.float32),
            jax.ShapeDtypeStruct((depth, share), bf),
        ),
        in_specs=[vm] * 2,
        out_specs=(vm, vm, vm),
        scratch_shapes=[
            pltpu.VMEM((dp, rows, cols), bf),
            pltpu.VMEM((2, GROUP, depth, share), bf),
            pltpu.VMEM((GROUP, depth, share), bf),
            pltpu.VMEM((GROUP, depth, share), bf),
            pltpu.VMEM((GROUP, depth, share), bf),
            pltpu.VMEM((GROUP - 1, depth, share), bf),
            dma(dp - 1), dma(dp - 1), dma(2 * GROUP), dma(2 * GROUP),
            dma(GROUP), dma(GROUP),
            dma(GROUP - 1), dma(GROUP - 1), pltpu.SemaphoreType.DMA,
        ],
        compiler_params=pltpu.CompilerParams(has_side_effects=True),
        name="collect",
    )(pk, yt)


def regrouped(dp, tp, inputs, cotangent, w_in, w_out, grad_in, grad_out):
    f32, bf = jnp.float32, jnp.bfloat16
    micro, toks, width = inputs.shape
    rows, hidden = w_in.shape
    part = hidden // GROUP
    scale_in = jnp.abs(w_in.astype(f32)) + ETA
    scale_out = jnp.abs(w_out.astype(f32)) + ETA
    scaled_in = scale_in * grad_in
    scaled_out = scale_out * grad_out
    partial_sq = jnp.sum(scaled_in * scaled_in) + jnp.sum(scaled_out * scaled_out)

    def pack(a, b):
        a = a.reshape(rows, GROUP, part)
        b = b.reshape(rows, GROUP, part)
        return jnp.concatenate([a, b], axis=2).transpose(1, 0, 2)

    pw = pack(w_in, w_out)
    pc = pack(RHO * scale_in * scaled_in, RHO * scale_out * scaled_out)
    count = micro * toks
    tx = inputs.reshape(tp, count // tp, width)
    tdy = cotangent.reshape(tp, count // tp, width)
    const = math.sqrt(2.0 * rows * dp * hidden * tp)
    wbuf, xbuf, dbuf, tot = spread(
        pw, pc, jnp.full((8, 128), partial_sq, f32), tx, tdy, dp, tp, const
    )
    factor = const / jnp.sqrt(tot[0, 0] + 1.0)
    ascent_in = factor * scaled_in
    ascent_out = factor * scaled_out
    full = wbuf.reshape(rows * dp, 2 * part)
    full_in, full_out = full[:, :part], full[:, part:]
    flat_x = xbuf.reshape(GROUP * count, width)
    flat_dy = dbuf.reshape(GROUP * count, width)

    def against(weight, tokens):
        return lax.dot_general(weight, tokens, (((0,), (1,)), ((), ())), preferred_element_type=f32)

    act, slope = gelu_parts(against(full_in, flat_x))
    act = act.astype(bf)
    yt = jnp.dot(full_out, act, preferred_element_type=f32)
    yt = yt.astype(bf).reshape(tp, width // tp, GROUP * count)
    delta = (against(full_out, flat_dy) * slope).astype(bf)
    packed = jnp.concatenate([
        jnp.dot(delta, flat_x, preferred_element_type=f32).astype(bf),
        jnp.dot(act, flat_dy, preferred_element_type=f32).astype(bf),
    ], axis=0).T.reshape(dp, rows, 2 * part)
    new_in, new_out, out = collect(packed, yt, dp, tp)
    branch = out.T.reshape(micro, toks, width // tp)
    return (branch, ascent_in, ascent_out, new_in, new_out)


def body(dp, tp, inputs, cotangent, w_in, *rest):
    micro, toks, width = inputs.shape
    rows, hidden = w_in.shape
    fits = (
        tp == 4 and dp % GROUP == 0 and rows % 16 == 0
        and hidden % (64 * GROUP) == 0 and (micro * toks) % 128 == 0
        and width % (32 * tp) == 0
    )
    if fits:
        return regrouped(dp, tp, inputs, cotangent, w_in, *rest)
    return local(inputs, cotangent, w_in, *rest)


def solution(mesh):
    return jax.shard_map(
        functools.partial(body, mesh.shape["dp"], mesh.shape["tensor"]),
        mesh=mesh,
        in_specs=(
            P(None, "dp", None),
            P(None, "dp", None),
            P("dp", "tensor"),
            P("dp", "tensor"),
            P("dp", "tensor"),
            P("dp", "tensor"),
        ),
        out_specs=(
            P(None, "dp", "tensor"),
            P("dp", "tensor"),
            P("dp", "tensor"),
            P("dp", "tensor"),
            P("dp", "tensor"),
        ),
        check_vma=False,
    )
```

```python
import functools
import math

import jax
import jax.numpy as jnp
from jax import lax
from jax.experimental import pallas as pl
from jax.experimental.pallas import tpu as pltpu
from jax.sharding import PartitionSpec as P

D = 1280
FF = 5120


RHO = 0.1
ETA = 0.01


def gelu_parts(pre):
    cdf = 0.5 * (1.0 + lax.erf(pre * 0.7071067811865476))
    dens = jnp.exp(-0.5 * pre * pre) * 0.3989422804014327
    return (pre * cdf, cdf + pre * dens)


def token_product(left, right):
    return lax.dot_general(
        left, right, (((0,), (0,)), ((), ())), preferred_element_type=jnp.float32
    )


def local(inputs, cotangent, w_in, w_out, grad_in, grad_out):
    scale_in = jnp.abs(w_in.astype(jnp.float32)) + ETA
    scale_out = jnp.abs(w_out.astype(jnp.float32)) + ETA
    scaled_in = scale_in * grad_in
    scaled_out = scale_out * grad_out
    partial_sq = jnp.sum(scaled_in * scaled_in) + jnp.sum(scaled_out * scaled_out)
    row_total = lax.psum(partial_sq, "tensor")
    total = lax.psum(row_total, "dp")
    factor = math.sqrt(2.0 * D * FF) / jnp.sqrt(total + 1.0)
    ascent_in = factor * scaled_in
    ascent_out = factor * scaled_out
    moved_in = (w_in.astype(jnp.float32) + RHO * scale_in * ascent_in).astype(jnp.bfloat16)
    moved_out = (w_out.astype(jnp.float32) + RHO * scale_out * ascent_out).astype(jnp.bfloat16)
    micro = inputs.shape[0]
    full_in, full_out = (
        lax.all_gather(moved_in, "dp", axis=0, tiled=True),
        lax.all_gather(moved_out, "dp", axis=0, tiled=True),
    )
    outputs = []
    acts = []
    deltas = []
    for index in range(micro):
        rows = inputs[index]
        grads_y = cotangent[index]
        pre = jnp.dot(rows, full_in, preferred_element_type=jnp.float32)
        act, slope = gelu_parts(pre)
        act = act.astype(jnp.bfloat16)
        partial_y = lax.dot_general(
            act, full_out, (((1,), (1,)), ((), ())), preferred_element_type=jnp.float32
        )
        shared_y = lax.psum_scatter(partial_y, "tensor", scatter_dimension=1, tiled=True)
        outputs.append(shared_y.astype(jnp.bfloat16))
        back = jnp.dot(grads_y, full_out, preferred_element_type=jnp.float32)
        acts.append(act)
        deltas.append((back * slope).astype(jnp.bfloat16))
    branch_output = jnp.stack(outputs)
    flat_x = inputs.reshape(-1, inputs.shape[2])
    flat_dy = cotangent.reshape(-1, cotangent.shape[2])
    flat_delta = jnp.concatenate(deltas, axis=0)
    flat_act = jnp.concatenate(acts, axis=0)
    whole_in = token_product(flat_x, flat_delta)
    whole_out = token_product(flat_dy, flat_act)
    new_in, new_out = (
        lax.psum_scatter(whole_in, "dp", scatter_dimension=0, tiled=True),
        lax.psum_scatter(whole_out, "dp", scatter_dimension=0, tiled=True),
    )
    return (branch_output, ascent_in, ascent_out, new_in, new_out)


MESH = pl.DeviceIdType.MESH
GROUP = 4


def remote(src, dst, send, recv, where):
    copy = pltpu.make_async_remote_copy(
        src_ref=src, dst_ref=dst, send_sem=send, recv_sem=recv,
        device_id=where, device_id_type=MESH,
    )
    copy.start()
    return copy


def spread_kernel(dp, tp, const, wi, wo, gi, go, tx, tdy, wbuf, xbuf, dbuf, tot,
                  sq, sb1, sb2, mid, mv, s1, r1, s2, r2, ws, wr, ts, tr, ys, yr, cs, cr, loc):
    d = lax.axis_index("dp")
    t = lax.axis_index("tensor")
    g = lax.rem(d, GROUP)
    base = d - g
    f32 = jnp.float32
    square = jnp.zeros((1, 1), f32)
    for w, grad in ((wi, gi), (wo, go)):
        scaled = (jnp.abs(w[...].astype(f32)) + ETA) * grad[...]
        square = square + jnp.sum(scaled * scaled, axis=(0, 1), keepdims=True)
    sq[...] = jnp.broadcast_to(square, sq.shape)
    copies = [
        remote(sq, sb1.at[k - 1], s1.at[k - 1], r1.at[k - 1], (d, lax.rem(t + k, tp)))
        for k in range(1, tp)
    ]
    pairs = ((tx, xbuf), (tdy, dbuf))
    own = [
        pltpu.make_async_copy(src, buf.at[g], loc.at[i]) for i, (src, buf) in enumerate(pairs)
    ]
    for copy in own:
        copy.start()
    for copy in copies:
        copy.wait()
    part = sq[...]
    for k in range(tp - 1):
        part = part + sb1[k]
    mid[...] = part
    copies = [
        remote(mid, sb2.at[k - 1], s2.at[k - 1], r2.at[k - 1], (lax.rem(d + k, dp), t))
        for k in range(1, dp)
    ]
    tokens = []
    for k in range(1, GROUP):
        p = lax.rem(g + k, GROUP)
        for i, (src, buf) in enumerate(pairs):
            n = 2 * k - 2 + i
            tokens.append(remote(src.at[t], buf.at[g, t], ts.at[n], tr.at[n], (base + p, t)))
    for copy in copies:
        copy.wait()
    for k in range(dp - 1):
        part = part + sb2[k]
    tot[...] = part
    factor = const / jnp.sqrt(part[0:1, 0:1] + 1.0)
    part_cols = wi.shape[1] // GROUP
    for j in range(GROUP):
        for i, (w, grad) in enumerate(((wi, gi), (wo, go))):
            weight = w[:, j * part_cols:(j + 1) * part_cols].astype(f32)
            scale = jnp.abs(weight) + ETA
            ascent = factor * (scale * grad[:, j * part_cols:(j + 1) * part_cols])
            mv[j, :, i * part_cols:(i + 1) * part_cols] = (
                weight + RHO * scale * ascent
            ).astype(jnp.bfloat16)
    own_w = pltpu.make_async_copy(mv.at[g], wbuf.at[d], loc.at[2])
    own_w.start()
    order = sorted(range(1, dp), key=lambda k: abs(2 * k - dp))
    weights = []

    def send_weight(k):
        e = lax.rem(d + k, dp)
        weights.append(remote(mv.at[lax.rem(e, GROUP)], wbuf.at[d],
                              ws.at[k - 1], wr.at[k - 1], (e, t)))

    for k in order:
        send_weight(k)
    ty = lax.rem(t + tp // 2, tp)
    tc = t + 1 - 2 * lax.rem(t, 2)
    across = []
    beside = []
    moves = 2 * GROUP - 2
    for n in range(moves):
        q = lax.rem(g + GROUP - (n // 2 + 1), GROUP)
        tokens[n].wait_recv()
        piece = pairs[n % 2][1].at[q, t]
        across.append(remote(piece, piece, ys.at[n], yr.at[n], (d, ty)))
        beside.append(remote(piece, piece, cs.at[n], cr.at[n], (d, tc)))
    for n in range(moves):
        q = lax.rem(g + GROUP - (n // 2 + 1), GROUP)
        across[n].wait_recv()
        piece = pairs[n % 2][1].at[q, ty]
        beside.append(remote(piece, piece, cs.at[moves + n], cr.at[moves + n], (d, tc)))
    for copy in tokens + across:
        copy.wait_send()
    for copy in weights + beside:
        copy.wait()
    for copy in own:
        copy.wait()
    own_w.wait()


def spread(w_in, w_out, grad_in, grad_out, tx, tdy, dp, tp, const):
    dma = lambda n: pltpu.SemaphoreType.DMA((n,))
    vm = pl.BlockSpec(memory_space=pltpu.VMEM)
    rows, hidden = w_in.shape
    group, cols = GROUP, 2 * hidden // GROUP
    return pl.pallas_call(
        functools.partial(spread_kernel, dp, tp, const),
        out_shape=(
            jax.ShapeDtypeStruct((dp, rows, cols), jnp.bfloat16),
            jax.ShapeDtypeStruct((group,) + tx.shape, jnp.bfloat16),
            jax.ShapeDtypeStruct((group,) + tdy.shape, jnp.bfloat16),
            jax.ShapeDtypeStruct((8, 128), jnp.float32),
        ),
        in_specs=[vm] * 6,
        out_specs=(vm, vm, vm, vm),
        scratch_shapes=[
            pltpu.VMEM((8, 128), jnp.float32),
            pltpu.VMEM((tp - 1, 8, 128), jnp.float32),
            pltpu.VMEM((dp - 1, 8, 128), jnp.float32),
            pltpu.VMEM((8, 128), jnp.float32),
            pltpu.VMEM((group, rows, cols), jnp.bfloat16),
            dma(tp - 1), dma(tp - 1), dma(dp - 1), dma(dp - 1), dma(dp - 1), dma(dp - 1),
            dma(2 * group - 2), dma(2 * group - 2), dma(2 * group - 2), dma(2 * group - 2),
            dma(4 * group - 4), dma(4 * group - 4), dma(3),
        ],
        compiler_params=pltpu.CompilerParams(has_side_effects=True),
        name="spread",
    )(w_in, w_out, grad_in, grad_out, tx, tdy)


def collect_kernel(dp, tp, pk, yt, new_in, new_out, out,
                   gbuf, cb, yst, yb, z3, zb, gs, gr, cs, cr, ys, yr, zs, zr, loc):
    d = lax.axis_index("dp")
    t = lax.axis_index("tensor")
    g = lax.rem(d, GROUP)
    base = d - g
    ty = lax.rem(t + tp // 2, tp)
    tc = t + 1 - 2 * lax.rem(t, 2)
    tcy = lax.rem(tc + tp // 2, tp)
    _, depth, share = yst.shape
    step = 32
    order = list(range(1, GROUP)) + [0]
    columns = [pl.ds(pl.multiple_of(lax.rem(g + k, GROUP) * share, share), share) for k in range(GROUP)]
    beside = [{}, {}]
    for half, whose in ((1, tcy), (0, tc)):
        for k in order:
            n = half * GROUP + k
            beside[half][k] = remote(
                yt.at[whose, :, columns[k]], cb.at[half, k], cs.at[n], cr.at[n], (d, tc)
            )
    sends = []
    for k in sorted(range(1, dp), key=lambda k: abs(2 * k - dp)):
        e = lax.rem(d + k, dp)
        sends.append(remote(pk.at[e], gbuf.at[d], gs.at[k - 1], gr.at[k - 1], (e, t)))
    f32 = jnp.float32
    own = pltpu.make_async_copy(pk.at[d], gbuf.at[d], loc)
    own.start()
    across = {}
    for k in order:
        beside[1][k].wait()

        @pl.loop(0, depth // step)
        def _(i):
            at = pl.ds(pl.multiple_of(i * step, step), step)
            whole = yt[ty, at, columns[k]].astype(f32) + cb[1, k, at, :].astype(f32)
            yst[k, at, :] = whole.astype(jnp.bfloat16)

        across[k] = remote(yst.at[k], yb.at[k], ys.at[k], yr.at[k], (d, ty))
    last = []
    for k in order:
        beside[0][k].wait()
        across[k].wait()

        @pl.loop(0, depth // step)
        def _(i):
            at = pl.ds(pl.multiple_of(i * step, step), step)
            whole = yt[t, at, columns[k]].astype(f32) + cb[0, k, at, :].astype(f32)
            z3[k, at, :] = (whole + yb[k, at, :].astype(f32)).astype(jnp.bfloat16)

        if k > 0:
            p = lax.rem(g + k, GROUP)
            last.append(remote(z3.at[k], zb.at[k - 1], zs.at[k - 1], zr.at[k - 1], (base + p, t)))
    for copy in sends:
        copy.wait()
    own.wait()
    part = pk.shape[2] // 2
    for j in range(GROUP):
        total = gbuf[j].astype(f32)
        for e in range(j + GROUP, dp, GROUP):
            total = total + gbuf[e].astype(f32)
        new_in[:, j * part:(j + 1) * part] = total[:, :part]
        new_out[:, j * part:(j + 1) * part] = total[:, part:]
    for copy in last:
        copy.wait()

    @pl.loop(0, depth // step)
    def _(i):
        at = pl.ds(pl.multiple_of(i * step, step), step)
        whole = z3[0, at, :].astype(f32)
        for k in range(GROUP - 1):
            whole = whole + zb[k, at, :].astype(f32)
        out[at, :] = whole.astype(jnp.bfloat16)


def collect(pk, yt, dp, tp):
    dma = lambda n: pltpu.SemaphoreType.DMA((n,))
    vm = pl.BlockSpec(memory_space=pltpu.VMEM)
    _, rows, cols = pk.shape
    _, depth, width = yt.shape
    share = width // GROUP
    bf = jnp.bfloat16
    return pl.pallas_call(
        functools.partial(collect_kernel, dp, tp),
        out_shape=(
            jax.ShapeDtypeStruct((rows, GROUP * cols // 2), jnp.float32),
            jax.ShapeDtypeStruct((rows, GROUP * cols // 2), jnp.float32),
            jax.ShapeDtypeStruct((depth, share), bf),
        ),
        in_specs=[vm] * 2,
        out_specs=(vm, vm, vm),
        scratch_shapes=[
            pltpu.VMEM((dp, rows, cols), bf),
            pltpu.VMEM((2, GROUP, depth, share), bf),
            pltpu.VMEM((GROUP, depth, share), bf),
            pltpu.VMEM((GROUP, depth, share), bf),
            pltpu.VMEM((GROUP, depth, share), bf),
            pltpu.VMEM((GROUP - 1, depth, share), bf),
            dma(dp - 1), dma(dp - 1), dma(2 * GROUP), dma(2 * GROUP),
            dma(GROUP), dma(GROUP),
            dma(GROUP - 1), dma(GROUP - 1), pltpu.SemaphoreType.DMA,
        ],
        compiler_params=pltpu.CompilerParams(has_side_effects=True),
        name="collect",
    )(pk, yt)


def regrouped(dp, tp, inputs, cotangent, w_in, w_out, grad_in, grad_out):
    f32, bf = jnp.float32, jnp.bfloat16
    micro, toks, width = inputs.shape
    rows, hidden = w_in.shape
    part = hidden // GROUP
    scale_in = jnp.abs(w_in.astype(f32)) + ETA
    scale_out = jnp.abs(w_out.astype(f32)) + ETA
    scaled_in = scale_in * grad_in
    scaled_out = scale_out * grad_out
    count = micro * toks
    tx = inputs.reshape(tp, count // tp, width)
    tdy = cotangent.reshape(tp, count // tp, width)
    const = math.sqrt(2.0 * rows * dp * hidden * tp)
    wbuf, xbuf, dbuf, tot = spread(
        w_in, w_out, grad_in, grad_out, tx, tdy, dp, tp, const
    )
    factor = const / jnp.sqrt(tot[0, 0] + 1.0)
    ascent_in = factor * scaled_in
    ascent_out = factor * scaled_out
    full = wbuf.reshape(rows * dp, 2 * part)
    full_in, full_out = full[:, :part], full[:, part:]
    flat_x = xbuf.reshape(GROUP * count, width)
    flat_dy = dbuf.reshape(GROUP * count, width)

    def against(weight, tokens):
        return lax.dot_general(weight, tokens, (((0,), (1,)), ((), ())), preferred_element_type=f32)

    act, slope = gelu_parts(against(full_in, flat_x))
    act = act.astype(bf)
    yt = jnp.dot(full_out, act, preferred_element_type=f32)
    yt = yt.astype(bf).reshape(tp, width // tp, GROUP * count)
    delta = (against(full_out, flat_dy) * slope).astype(bf)
    packed = jnp.concatenate([
        jnp.dot(delta, flat_x, preferred_element_type=f32).astype(bf),
        jnp.dot(act, flat_dy, preferred_element_type=f32).astype(bf),
    ], axis=0).T.reshape(dp, rows, 2 * part)
    new_in, new_out, out = collect(packed, yt, dp, tp)
    branch = out.T.reshape(micro, toks, width // tp)
    return (branch, ascent_in, ascent_out, new_in, new_out)


def body(dp, tp, inputs, cotangent, w_in, *rest):
    micro, toks, width = inputs.shape
    rows, hidden = w_in.shape
    fits = (
        tp == 4 and dp % GROUP == 0 and rows % 16 == 0
        and hidden % (64 * GROUP) == 0 and (micro * toks) % 128 == 0
        and width % (32 * tp) == 0
    )
    if fits:
        return regrouped(dp, tp, inputs, cotangent, w_in, *rest)
    return local(inputs, cotangent, w_in, *rest)


def solution(mesh):
    return jax.shard_map(
        functools.partial(body, mesh.shape["dp"], mesh.shape["tensor"]),
        mesh=mesh,
        in_specs=(
            P(None, "dp", None),
            P(None, "dp", None),
            P("dp", "tensor"),
            P("dp", "tensor"),
            P("dp", "tensor"),
            P("dp", "tensor"),
        ),
        out_specs=(
            P(None, "dp", "tensor"),
            P("dp", "tensor"),
            P("dp", "tensor"),
            P("dp", "tensor"),
            P("dp", "tensor"),
        ),
        check_vma=False,
    )
```
